128 devices in a mesh: groups: 4 (over x, y), seq: 32 (over z, core).
Axes of the slice: x: 2, y: 2, z: 16, core: 2. Of those that a mesh axis runs over, the one named last changes fastest.
The devices are a block of a 8x8x16 slice.
Arguments:
- candidates: bfloat16 [64, 512, 256], P('groups', 'seq'), parts along dimension 0, may hold values from -110 to 110
- codes: int32 [64, 4096, 256], P('groups', 'seq'), parts along dimension 0, may hold values from -2147483648 to 2147483647
- scale_index: int32 [64, 16384], P('groups', 'seq'), parts along dimension 0, may hold values from 0 to 255
- lengths: int32 [64], P('groups'), parts along dimension 0, may hold values from 128 to 16384, as said below
- scale_table: float32 [256], replicated, may hold values from 0.004 to 0.04
- query_weight: bfloat16 [256, 256], replicated, may hold values from -0.375 to 0.375
- key_weight: bfloat16 [256, 256], replicated, may hold values from -0.375 to 0.375
- value_weight: bfloat16 [256, 256], replicated, may hold values from -0.375 to 0.375
- out_weight: bfloat16 [256, 256], replicated, may hold values from -0.375 to 0.375
- norm_gain: float32 [256], replicated, may hold values from 0.1 to 1.9
- hidden_weight: bfloat16 [256, 512], replicated, may hold values from -0.375 to 0.375
- hidden_bias: float32 [512], replicated, may hold values from -4 to 4
- score_weight: bfloat16 [512], replicated, may hold values from -0.25 to 0.25
Outputs:
- interest: bfloat16 [64, 512, 256], P('groups', 'seq'), parts along dimension 0
- logits: float32 [64, 512], P('groups', 'seq'), parts along dimension 0
The draws below stay inside these ranges and needn't reach their ends.
There are 4 independent parts, one for each index of `groups`. The reference program is written for one: setup_inputs(seed, part) draws one part's arguments, and reference() takes and returns one part's arrays. A program takes and returns all parts, laid end to end along the dimension named above; an argument that names none is the same for every part. Nothing has to cross between parts.
Inputs may be any that keep to these rules, and one draw needn't show every extreme that they name: `lengths`: each user's history length is a multiple of 128; in every draw some user's length is 16384.
All inputs are finite; a program needn't handle non-finite values.
Results may differ from the reference program's by a relative error of at most 0.02.
The reference program's roundings to bfloat16 on the way count: a program that leaves them out, or rounds other values in their place, can miss the bound.
Values may be sent and summed in bfloat16 or wider, within the bound.
No kernel may reach another device: no remote copies, remote signals or barrier semaphores. Data moves between devices by JAX's collectives and lax.ppermute only.
A program may use at most 128 MiB of HBM per device.

```python
import math
import jax
import jax.numpy as jnp
from jax import lax

WIDTH = 256
HEADS = 4
RANK_HIDDEN = 512
LEVELS = 256
LGRAIN = 128
USERS = 16
CAND = 512
HIST = 16384


def draw_candidates(key, part):
    base_key = jax.random.fold_in(jax.random.fold_in(key, 5), 0)
    scale_key = jax.random.fold_in(jax.random.fold_in(key, 5), 1)
    class_key = jax.random.fold_in(jax.random.fold_in(key, 5), 2)
    weak_key = jax.random.fold_in(jax.random.fold_in(key, 5), 4)
    shape = (USERS, CAND, WIDTH)
    row_class = jax.random.uniform(class_key, (USERS, CAND, 1), jnp.float32)
    weak = jnp.exp(jax.random.uniform(weak_key, (USERS, CAND, 1), jnp.float32, math.log(0.05), math.log(0.3)))
    medium = jnp.exp(jax.random.uniform(scale_key, (USERS, CAND, 1), jnp.float32, math.log(1.5), math.log(7.0)))
    values = jnp.clip(jax.random.normal(base_key, shape, jnp.float32), -6.0, 6.0)
    row_scales = jnp.where(row_class < 0.5, weak, medium)
    return (values * row_scales).astype(jnp.bfloat16)


def draw_codes(key, part):
    tilt_key, regime_key, sign_key, high_key, low_key, full_key = jax.random.split(jax.random.fold_in(key, 7), 6)
    word_count = HIST // 4
    block_count = HIST // LGRAIN
    shape = (USERS, word_count, WIDTH)
    tilt = jax.random.randint(tilt_key, (USERS, 1), 0, 4)
    regime = jax.random.randint(regime_key, (USERS, block_count), 0, 3)
    regime = jnp.where(tilt == 0, 0, regime)
    per_word = jnp.repeat(regime, LGRAIN // 4, axis=1)[:, :, None]
    packed = jnp.zeros(shape, jnp.int32)
    for k in range(4):
        signs = jax.random.randint(jax.random.fold_in(sign_key, k), shape, 0, 2) * 2 - 1
        high = signs * jax.random.randint(jax.random.fold_in(high_key, k), shape, 100, 128)
        low = jax.random.randint(jax.random.fold_in(low_key, k), shape, -12, 13)
        full = jax.random.randint(jax.random.fold_in(full_key, k), shape, -128, 128)
        byte_value = jnp.where(per_word == 2, high, jnp.where(per_word == 1, full, low)).astype(jnp.int32)
        packed = jnp.bitwise_or(packed, jnp.left_shift(jnp.bitwise_and(byte_value, 255), 8 * k))
    return packed


def draw_lengths(key, part):
    first_key, second_key = jax.random.split(jax.random.fold_in(key, 11))
    granules = jax.random.randint(first_key, (USERS,), 1, HIST // LGRAIN + 1)
    longest = jax.random.randint(second_key, (), 0, USERS)
    granules = jnp.where(jnp.arange(USERS, dtype=jnp.int32) == longest, HIST // LGRAIN, granules)
    return (granules * LGRAIN).astype(jnp.int32)


def set_ends(values, stream_key, low, top_value):
    dims = values.shape
    index_at = [jax.random.randint(jax.random.fold_in(stream_key, axis), (), 0, dims[axis]) for axis in range(len(dims))]
    values = values.at[tuple(index_at)].set(low)
    longest = dims.index(max(dims))
    index_at[longest] = (index_at[longest] + 1) % dims[longest]
    return values.at[tuple(index_at)].set(top_value)


def centred(stream_key, extent, width, limit, kind=jnp.bfloat16):
    values = jax.random.normal(stream_key, extent, jnp.float32) * width
    return jnp.minimum(jnp.maximum(values, -limit), limit).astype(kind)


def setup_inputs(seed: int = 0, part: int = 0) -> dict:
    arg_keys = jax.random.split(jax.random.key(seed), 14)
    part_keys = jax.random.split(jax.random.fold_in(arg_keys[13], part), 14)
    candidates = draw_candidates(jax.random.fold_in(jax.random.fold_in(arg_keys[13], part), 71), part)
    codes = draw_codes(jax.random.fold_in(jax.random.fold_in(arg_keys[13], part), 71), part)
    scale_index = set_ends(jax.random.randint(part_keys[2], (USERS, HIST), 0, LEVELS), jax.random.fold_in(part_keys[2], 1), 0, LEVELS - 1).astype(jnp.int32)
    lengths = draw_lengths(jax.random.fold_in(jax.random.fold_in(arg_keys[13], part), 71), part)
    scale_table = jnp.clip(jnp.exp(jax.random.uniform(arg_keys[4], (LEVELS,), jnp.float32, math.log(0.004), math.log(0.04))), 0.004, 0.04)
    query_weight = centred(arg_keys[5], (WIDTH, WIDTH), WIDTH ** -0.5, 0.375)
    key_weight = centred(arg_keys[6], (WIDTH, WIDTH), WIDTH ** -0.5, 0.375)
    value_weight = centred(arg_keys[7], (WIDTH, WIDTH), WIDTH ** -0.5, 0.375)
    out_weight = centred(arg_keys[8], (WIDTH, WIDTH), WIDTH ** -0.5, 0.375)
    norm_gain = jnp.clip(1.0 + 0.18 * jax.random.normal(arg_keys[9], (WIDTH,), jnp.float32), 0.1, 1.9)
    hidden_weight = centred(arg_keys[10], (WIDTH, RANK_HIDDEN), WIDTH ** -0.5, 0.375)
    hidden_bias = centred(arg_keys[11], (RANK_HIDDEN,), 1.0, 4.0, jnp.float32)
    score_weight = centred(arg_keys[12], (RANK_HIDDEN,), RANK_HIDDEN ** -0.5, 0.25)
    return dict(candidates=candidates, codes=codes, scale_index=scale_index, lengths=lengths, scale_table=scale_table, query_weight=query_weight, key_weight=key_weight, value_weight=value_weight, out_weight=out_weight, norm_gain=norm_gain, hidden_weight=hidden_weight, hidden_bias=hidden_bias, score_weight=score_weight)


NEG_FILL = -1e+30

def unpack_codes(words):
    byte_rows = [jnp.right_shift(jnp.left_shift(words, 24 - 8 * k), 24) for k in range(4)]
    stacked = jnp.stack(byte_rows, axis=1)
    return stacked.reshape(words.shape[0] * 4, words.shape[1])

def reference(candidates, codes, scale_index, lengths, scale_table, query_weight, key_weight, value_weight, out_weight, norm_gain, hidden_weight, hidden_bias, score_weight):
    head_size = WIDTH // HEADS
    inv_root = 1.0 / math.sqrt(head_size)
    positions = jnp.arange(HIST, dtype=jnp.int32)

    def one_user(user_item):
        cand_rows, word_rows, index_rows, user_length = user_item
        code_rows = unpack_codes(word_rows)
        history = (code_rows.astype(jnp.float32) * scale_table[index_rows][:, None]).astype(jnp.bfloat16)
        all_keys = jnp.dot(history, key_weight, preferred_element_type=jnp.float32).astype(jnp.bfloat16)
        all_values = jnp.dot(history, value_weight, preferred_element_type=jnp.float32).astype(jnp.bfloat16)
        queries = jnp.dot(cand_rows, query_weight, preferred_element_type=jnp.float32).astype(jnp.bfloat16)
        live_mask = positions < user_length

        def one_head(head_index):
            start = (head_index * head_size).astype(jnp.int32)
            query_head = lax.dynamic_slice_in_dim(queries, start, head_size, 1)
            key_head = lax.dynamic_slice_in_dim(all_keys, start, head_size, 1)
            value_head = lax.dynamic_slice_in_dim(all_values, start, head_size, 1)
            scores = jnp.dot(query_head, key_head.T, preferred_element_type=jnp.float32) * inv_root
            scores = jnp.where(live_mask[None, :], scores, NEG_FILL)
            peak_rows = lax.optimization_barrier(jnp.max(scores, axis=1, keepdims=True))
            weights = jnp.where(live_mask[None, :], jnp.exp(scores - peak_rows), 0.0)
            totals = lax.optimization_barrier(jnp.sum(weights, axis=1, keepdims=True))
            numerators = jnp.dot(weights.astype(jnp.bfloat16), value_head, preferred_element_type=jnp.float32)
            return numerators / totals
        head_outs = lax.map(one_head, jnp.arange(HEADS, dtype=jnp.int32))
        attended = jnp.transpose(head_outs, (1, 0, 2)).reshape(CAND, WIDTH).astype(jnp.bfloat16)
        interest = jnp.dot(attended, out_weight, preferred_element_type=jnp.float32).astype(jnp.bfloat16)
        floats = interest.astype(jnp.float32)
        normed = (floats * lax.rsqrt(lax.optimization_barrier(jnp.mean(floats * floats, axis=1, keepdims=True)) + 1e-06) * norm_gain).astype(jnp.bfloat16)
        hidden = jax.nn.silu(jnp.dot(normed, hidden_weight, preferred_element_type=jnp.float32) + hidden_bias).astype(jnp.bfloat16)
        logits = jnp.dot(hidden, score_weight, preferred_element_type=jnp.float32)
        return (interest, logits)
    interest, logits = lax.map(one_user, (candidates, codes, scale_index, lengths))
    return (interest, logits)
```

```python
import functools

import jax
import jax.numpy as jnp
from jax import lax
from jax.experimental import pallas as pl
from jax.experimental.pallas import tpu as pltpu
from jax.sharding import PartitionSpec as P

HEADS = 4
GRAIN = 128
BYTES = 4
NEG = -1e30
SPAN = 4
GROUP = 4
STATS = 16
ONES = 16
BATCH = 4

NT = (((1,), (1,)), ((), ()))
TN = (((0,), (0,)), ((), ()))


def dot(a, b, dims=(((1,), (0,)), ((), ()))):
    return lax.dot_general(a, b, dims, preferred_element_type=jnp.float32)


def cost(flops, moved):
    return pl.CostEstimate(flops=int(flops), bytes_accessed=int(moved), transcendentals=0)


def history_body(words, index, table, out):
    levels = table.shape[1]
    words_per = GRAIN // BYTES
    spot = lax.broadcasted_iota(jnp.int32, (GRAIN, GRAIN), 0)
    place = lax.broadcasted_iota(jnp.int32, (GRAIN, GRAIN), 1)
    moves = (spot == BYTES * (place % words_per) + place // words_per).astype(jnp.bfloat16)
    level = lax.broadcasted_iota(jnp.int32, (levels, GRAIN), 0).astype(jnp.float32)
    entry = jnp.broadcast_to(table[...], (GRAIN, levels)).T
    users = words.shape[0]
    first = pl.program_id(0) * users
    for u in range(users):
        indices = index[pl.ds(first + u, 1), :].astype(jnp.float32)
        for g in range(words.shape[1] // words_per):
            row = indices[:, g * GRAIN : (g + 1) * GRAIN]
            row = jnp.broadcast_to(row, (16, GRAIN)).astype(jnp.bfloat16)
            row = dot(row, moves)[0:1]
            scales = jnp.sum(jnp.where(level == row, entry, 0.0), axis=0, keepdims=True)
            scales = jnp.broadcast_to(scales, (GRAIN, GRAIN)).T
            block = words[u, g * words_per : (g + 1) * words_per, :]
            for k in range(BYTES):
                codes = jnp.right_shift(jnp.left_shift(block, 24 - 8 * k), 24).astype(jnp.float32)
                part = scales[k * words_per : (k + 1) * words_per]
                part = jnp.concatenate([part] * (block.shape[1] // GRAIN), axis=1)
                start = g * GRAIN + k * words_per
                out[u, start : start + words_per, :] = (codes * part).astype(jnp.bfloat16)


def history_rows(codes, scale_index, scale_table):
    users, words, width = codes.shape
    places = words * BYTES
    levels = scale_table.shape[0]
    return pl.pallas_call(
        history_body,
        grid=(users // BATCH,),
        in_specs=[
            pl.BlockSpec((BATCH, words, width), lambda u: (u, 0, 0)),
            pl.BlockSpec((users, places), lambda u: (0, 0)),
            pl.BlockSpec((1, levels), lambda u: (0, 0)),
        ],
        out_specs=pl.BlockSpec((BATCH, places, width), lambda u: (u, 0, 0)),
        out_shape=jax.ShapeDtypeStruct((users, places, width), jnp.bfloat16),
        cost_estimate=cost(2e9, 6e6),
        name="history",
    )(codes, scale_index, scale_table.reshape(1, levels))


def project_body(rows, key_w, value_wt, keys, values):
    width = key_w.shape[0]
    half = width // 2
    for u in range(rows.shape[0]):
        h = rows[u]
        keys[u] = dot(h, key_w[...]).astype(jnp.bfloat16)
        v = dot(value_wt[...], h, NT).astype(jnp.bfloat16)
        ones = jnp.ones((ONES, h.shape[0]), jnp.bfloat16)
        for p in range(2):
            at = p * (half + ONES)
            values[u, at : at + half, :] = v[p * half : (p + 1) * half]
            values[u, at + half : at + half + ONES, :] = ones


def project(rows, key_w, value_wt):
    users, places, width = rows.shape
    tall = width + 2 * ONES
    return pl.pallas_call(
        project_body,
        grid=(users // BATCH,),
        in_specs=[
            pl.BlockSpec((BATCH, places, width), lambda u: (u, 0, 0)),
            pl.BlockSpec((width, width), lambda u: (0, 0)),
            pl.BlockSpec((width, width), lambda u: (0, 0)),
        ],
        out_specs=[
            pl.BlockSpec((BATCH, places, width), lambda u: (u, 0, 0)),
            pl.BlockSpec((BATCH, tall, places), lambda u: (u, 0, 0)),
        ],
        out_shape=[
            jax.ShapeDtypeStruct((users, places, width), jnp.bfloat16),
            jax.ShapeDtypeStruct((users, tall, places), jnp.bfloat16),
        ],
        cost_estimate=cost(3e9, 12e6),
        name="project",
    )(rows, key_w, value_wt)


def query_body(rows, weight, out):
    head = weight.shape[1] // HEADS
    q = dot(rows[...], weight[...]).astype(jnp.bfloat16)
    out[...] = q * jnp.bfloat16(head**-0.5)


def query_rows(rows, weight):
    return pl.pallas_call(
        query_body,
        out_shape=jax.ShapeDtypeStruct((rows.shape[0], weight.shape[1]), jnp.bfloat16),
        cost_estimate=cost(3e7, 4e5),
        name="query",
    )(rows, weight)


def parts_of(peak):
    hi = peak.astype(jnp.bfloat16).astype(jnp.float32)
    mid = (peak - hi).astype(jnp.bfloat16).astype(jnp.float32)
    return [hi, mid, peak - hi - mid]


def attend_user(user, k, pieces, live, k_own, k_other, v_own, v_other, scores, weights, held, at):
    width = k_own.shape[2]
    head = width // HEADS
    pair = 2 * head
    counts = (live[0, user], live[1, user])
    per = k_own.shape[1] // GRAIN
    lanes = held.shape[1] // GROUP

    @pl.when(counts[0] + counts[1] == 0)
    def _():
        held[0:width, at] = jnp.zeros((width, lanes), jnp.bfloat16)
        row = lax.broadcasted_iota(jnp.int32, (STATS, lanes), 0)
        held[width : width + STATS, at] = jnp.where(row < HEADS, NEG, 0.0).astype(jnp.bfloat16)

    @pl.when(counts[0] + counts[1] > 0)
    def _():
        q = jnp.concatenate([r[user] for r in pieces], axis=0)
        lane = lax.broadcasted_iota(jnp.int32, (lanes, pair), 1)
        peaks, totals = [], []
        for p in range(HEADS // 2):
            both = q[:, p * pair : (p + 1) * pair].astype(jnp.float32)
            right = jnp.concatenate(
                [jnp.where(lane < head, both, 0.0), jnp.where(lane < head, 0.0, both)], axis=0
            ).astype(jnp.bfloat16)
            tops = []
            for t in range(2 * per):
                source, place = ((k_own, t), (k_other, t - per))[t >= per]
                s = dot(source[k, place * GRAIN : (place + 1) * GRAIN, p * pair : (p + 1) * pair], right, NT)
                scores[p, t * GRAIN : (t + 1) * GRAIN, :] = s
                alive = place < counts[t >= per]
                tops.append(jnp.where(alive, jnp.max(s, axis=0, keepdims=True), NEG))
            peaks.append(functools.reduce(jnp.maximum, tops))
        for p in range(HEADS // 2):
            for t in range(2 * per):
                alive = t % per < counts[t >= per]
                lift = jnp.where(alive, peaks[p], -NEG)
                w = jnp.exp(scores[p, t * GRAIN : (t + 1) * GRAIN, :] - lift)
                weights[p, t * GRAIN : (t + 1) * GRAIN, :] = w.astype(jnp.bfloat16)
            rows = slice(p * (pair + ONES), (p + 1) * (pair + ONES))
            half = per * GRAIN
            o = dot(v_own[k, rows, :], weights[p, 0:half, :]) + dot(v_other[k, rows, :], weights[p, half : 2 * half, :])
            held[p * pair : p * pair + head, at] = o[0:head, 0:lanes].astype(jnp.bfloat16)
            held[p * pair + head : (p + 1) * pair, at] = o[head:pair, lanes:].astype(jnp.bfloat16)
            totals += [o[pair : pair + 1, 0:lanes], o[pair : pair + 1, lanes:]]
        peak = jnp.concatenate([x for p in peaks for x in (p[:, 0:lanes], p[:, lanes:])], axis=0)
        stats = jnp.concatenate(parts_of(peak) + totals, axis=0)
        held[width : width + STATS, at] = stats.astype(jnp.bfloat16)


def attend_body(base, live, *refs):
    pieces, refs = refs[: 2 * SPAN], refs[2 * SPAN :]
    (k_own, k_other, v_own, v_other, order), refs = refs[:5], refs[5:]
    outs, (scores, weights, held) = refs[:SPAN], refs[SPAN:]
    lanes = held.shape[1] // GROUP
    batch = k_own.shape[0]
    i = pl.program_id(1)
    for k in range(batch):
        place = i * batch + k
        user = base + pl.program_id(0) * GROUP + place
        at = pl.ds(pl.multiple_of(place * lanes, lanes), lanes)
        attend_user(user, k, pieces, live, k_own, k_other, v_own, v_other, scores, weights, held, at)

    @pl.when(i == GROUP // batch - 1)
    def _():
        mixed = dot(held[...], order[...]).astype(jnp.bfloat16)
        for s in range(SPAN):
            outs[s][...] = mixed[:, s * lanes : (s + 1) * lanes]


def attend(base, users, live, pieces, k_own, k_other, v_own, v_other, order):
    cand, width = pieces[0].shape[1:]
    places = k_own.shape[1]
    tall = v_own.shape[1]
    lanes = cand * len(pieces)
    deep = width + STATS
    batch = 2
    steps = GROUP // batch
    some = lambda g, i, live: (base // batch + g * steps + i, 0, 0)
    flat = lambda g, i, live: (0, 0)
    return pl.pallas_call(
        functools.partial(attend_body, base),
        grid_spec=pltpu.PrefetchScalarGridSpec(
            num_scalar_prefetch=1,
            grid=(users // GROUP, steps),
            in_specs=[pl.BlockSpec(memory_space=pltpu.VMEM) for _ in pieces]
            + [
                pl.BlockSpec((batch, places, width), some),
                pl.BlockSpec((batch, places, width), some),
                pl.BlockSpec((batch, tall, places), some),
                pl.BlockSpec((batch, tall, places), some),
                pl.BlockSpec(memory_space=pltpu.VMEM),
            ],
            out_specs=[pl.BlockSpec((deep, lanes), lambda g, i, live: (0, g))] * SPAN,
            scratch_shapes=[
                pltpu.VMEM((HEADS // 2, 2 * places, 2 * lanes), jnp.float32),
                pltpu.VMEM((HEADS // 2, 2 * places, 2 * lanes), jnp.bfloat16),
                pltpu.VMEM((deep, GROUP * lanes), jnp.bfloat16),
            ],
        ),
        out_shape=[jax.ShapeDtypeStruct((deep, users * lanes // SPAN), jnp.bfloat16)] * SPAN,
        cost_estimate=cost(6e9, 9e6),
        name="attend",
    )(live, *pieces, k_own, k_other, v_own, v_other, order)


def merged(a, b):
    width = a.shape[0] - STATS
    head = width // HEADS
    sa, sb = a[width:].astype(jnp.float32), b[width:].astype(jnp.float32)
    pa = sa[0:4] + sa[4:8] + sa[8:12]
    pb = sb[0:4] + sb[4:8] + sb[8:12]
    peak = jnp.maximum(pa, pb)
    fa, fb = jnp.exp(pa - peak), jnp.exp(pb - peak)
    total = fa * sa[12:16] + fb * sb[12:16]
    rows = []
    for h in range(HEADS):
        na = a[h * head : (h + 1) * head].astype(jnp.float32)
        nb = b[h * head : (h + 1) * head].astype(jnp.float32)
        rows.append(na * fa[h : h + 1] + nb * fb[h : h + 1])
    return rows, peak, total


def packed(rows, peak, total):
    stats = jnp.concatenate(parts_of(peak) + [total], axis=0)
    return jnp.concatenate([r.astype(jnp.bfloat16) for r in rows] + [stats.astype(jnp.bfloat16)], axis=0)


def merge_body(came, mine, out):
    out[...] = packed(*merged(came[...], mine[...]))


def merge(came, mine):
    return pl.pallas_call(
        merge_body,
        out_shape=jax.ShapeDtypeStruct(came.shape, jnp.bfloat16),
        cost_estimate=cost(1e8, 5e5),
        name="merge",
    )(came, mine)


def split_body(came_a, came_b, mine_a, mine_b, order, near, far):
    lanes = came_a.shape[1] // 2
    for n, (came, mine) in enumerate(((came_a, mine_a), (came_b, mine_b))):
        both = dot(packed(*merged(came[...], mine[...])), order[...]).astype(jnp.bfloat16)
        near[:, n * lanes : (n + 1) * lanes] = both[:, 0:lanes]
        far[:, n * lanes : (n + 1) * lanes] = both[:, lanes:]


def split(came_a, came_b, mine_a, mine_b, order):
    return pl.pallas_call(
        split_body,
        out_shape=[jax.ShapeDtypeStruct(came_a.shape, jnp.bfloat16)] * 2,
        cost_estimate=cost(1e8, 1e6),
        name="split",
    )(came_a, came_b, mine_a, mine_b, order)


def finish_body(a, b, out_w, gain, hidden_w, bias, score_w, interest, logits):
    rows, _, total = merged(a[...], b[...])
    attended = jnp.concatenate(
        [(r / total[h : h + 1]).astype(jnp.bfloat16) for h, r in enumerate(rows)], axis=0
    )
    found = dot(attended, out_w[...], TN).astype(jnp.bfloat16)
    interest[...] = found
    f = found.astype(jnp.float32)
    normed = f * lax.rsqrt(jnp.mean(f * f, axis=1, keepdims=True) + 1e-6) * gain[...]
    v = dot(normed.astype(jnp.bfloat16), hidden_w[...]) + bias[...]
    hidden = (v / (1.0 + jnp.exp(-v))).astype(jnp.bfloat16)
    row = dot(jnp.broadcast_to(score_w[...], (16, v.shape[1])), hidden, NT)[0:1]
    users, cand = logits.shape
    lane = lax.broadcasted_iota(jnp.int32, (users, users * cand), 1)
    mine = lane // cand == lax.broadcasted_iota(jnp.int32, (users, users * cand), 0)
    fold = lax.broadcasted_iota(jnp.int32, (users * cand, cand), 0) % cand
    fold = (fold == lax.broadcasted_iota(jnp.int32, (users * cand, cand), 1)).astype(jnp.bfloat16)
    folded = [dot(jnp.where(mine, r, 0.0).astype(jnp.bfloat16), fold) for r in parts_of(row)]
    logits[...] = folded[0] + folded[1] + folded[2]


def finish(users, a, b, out_w, gain, hidden_w, bias, score_w):
    width, wide = hidden_w.shape
    lanes = a.shape[1]
    return pl.pallas_call(
        finish_body,
        out_shape=[
            jax.ShapeDtypeStruct((lanes, width), jnp.bfloat16),
            jax.ShapeDtypeStruct((users, lanes // users), jnp.float32),
        ],
        cost_estimate=cost(2e8, 1e6),
        name="finish",
    )(a, b, out_w, gain.reshape(1, width), hidden_w, bias.reshape(1, wide), score_w.reshape(1, wide))


def reorder(shape, axes):
    size = 1
    for n in shape:
        size *= n
    spot = lax.broadcasted_iota(jnp.int32, (size, size), 1)
    dims = [shape[a] for a in axes]
    digits = []
    for n in reversed(dims):
        digits.insert(0, spot % n)
        spot = spot // n
    source = 0
    for a, n in enumerate(shape):
        source = source * n + digits[axes.index(a)]
    return (lax.broadcasted_iota(jnp.int32, (size, size), 0) == source).astype(jnp.bfloat16)


def solution(mesh):
    peers = mesh.shape["seq"]
    chips = peers // 2
    slots = chips // 2
    near = lambda d, c: (d % chips) * 2 + c
    ring = [(near(d, 0), near(d + 1, 0)) for d in range(chips)] + [(near(d, 1), near(d - 1, 1)) for d in range(chips)]
    stay = [(near(d, 0), near(d, 0)) for d in range(chips)] + [(near(d, 1), near(d - 1, 1)) for d in range(chips)]
    cross = [(near(d, 1), near(d, 0)) for d in range(chips)] + [(near(d, 0), near(d - 1, 1)) for d in range(chips)]
    swap = [(near(d, c), near(d, 1 - c)) for d in range(chips) for c in range(2)]
    back = lambda pairs: [(b, a) for a, b in pairs]

    def on_device(
        candidates,
        codes,
        scale_index,
        lengths,
        scale_table,
        query_weight,
        key_weight,
        value_weight,
        out_weight,
        norm_gain,
        hidden_weight,
        hidden_bias,
        score_weight,
    ):
        users, cand, width = candidates.shape
        places = scale_index.shape[1]
        send = lambda array, pairs: lax.ppermute(array, "seq", pairs)
        me = lax.axis_index("seq")
        mate = me + 1 - 2 * (me % 2)
        starts = jnp.stack([me, mate])[:, None] * places
        live = jnp.clip((lengths[None, :] - starts) // GRAIN, 0, places // GRAIN).astype(jnp.int32)

        mine = query_rows(candidates.reshape(users * cand, width), query_weight).reshape(users, cand, width)
        chunks = [(send(mine, stay), send(mine, cross))]
        for _ in range(slots - 1):
            chunks.append(tuple(send(c, ring) for c in chunks[-1]))

        value_wt = value_weight.T
        own = history_rows(codes, scale_index, scale_table)
        other = send(own, swap)
        k_own, v_own = project(own, key_weight, value_wt)
        k_other, v_other = project(other, key_weight, value_wt)

        order = reorder((GROUP, SPAN, 2 * cand), (1, 0, 2))
        half = users // 2
        partial = [[], []]
        for block in range(slots // SPAN):
            pieces = [c for pair in chunks[block * SPAN : (block + 1) * SPAN] for c in pair]
            for part in range(2):
                partial[part] += attend(part * half, half, live, pieces, k_own, k_other, v_own, v_other, order)

        come = [p[-1] for p in partial]
        for slot in range(slots - 2, -1, -1):
            come = [send(c, back(ring)) for c in come]
            if slot:
                come = [merge(c, p[slot]) for c, p in zip(come, partial)]
        halves = reorder((half, 2, cand), (1, 0, 2))
        first, second = split(*come, partial[0][0], partial[1][0], halves)
        first, second = send(first, back(stay)), send(second, back(cross))
        interest, logits = finish(
            users, first, second, out_weight, norm_gain, hidden_weight, hidden_bias, score_weight
        )
        return interest.reshape(users, cand, width), logits

    in_specs = (
        P("groups", "seq", None),
        P("groups", "seq", None),
        P("groups", "seq"),
        P("groups"),
    ) + (P(),) * 9
    out_specs = (P("groups", "seq", None), P("groups", "seq"))
    return jax.shard_map(on_device, mesh=mesh, in_specs=in_specs, out_specs=out_specs, check_vma=False)
```

```python
import functools

import jax
import jax.numpy as jnp
from jax import lax
from jax.experimental import pallas as pl
from jax.experimental.pallas import tpu as pltpu
from jax.sharding import PartitionSpec as P


HEADS = 4
GRAIN = 128
BYTES = 4
NEG = -1e30
SPAN = 4
GROUP = 4
STATS = 16
ONES = 16
PARTS = 2
BATCH = 4
FULL = 62.5

NT = (((1,), (1,)), ((), ()))
TN = (((0,), (0,)), ((), ()))


def dot(a, b, dims=(((1,), (0,)), ((), ()))):
    return lax.dot_general(a, b, dims, preferred_element_type=jnp.float32)


def cost(flops, moved):
    return pl.CostEstimate(flops=int(flops), bytes_accessed=int(moved), transcendentals=0)


def room(mib):
    return pltpu.CompilerParams(vmem_limit_bytes=int(mib * 2**20))


def history_body(words, index, table, out):
    levels = table.shape[1]
    words_per = GRAIN // BYTES
    spot = lax.broadcasted_iota(jnp.int32, (GRAIN, GRAIN), 0)
    place = lax.broadcasted_iota(jnp.int32, (GRAIN, GRAIN), 1)
    moves = (spot == BYTES * (place % words_per) + place // words_per).astype(jnp.bfloat16)
    level = lax.broadcasted_iota(jnp.int32, (levels, GRAIN), 0).astype(jnp.float32)
    entry = jnp.broadcast_to(table[...], (GRAIN, levels)).T
    users = words.shape[0]
    first = pl.program_id(0) * users
    for u in range(users):
        indices = index[pl.ds(first + u, 1), :].astype(jnp.float32)
        for g in range(words.shape[1] // words_per):
            row = indices[:, g * GRAIN : (g + 1) * GRAIN]
            row = jnp.broadcast_to(row, (16, GRAIN)).astype(jnp.bfloat16)
            row = dot(row, moves)[0:1]
            scales = jnp.sum(jnp.where(level == row, entry, 0.0), axis=0, keepdims=True)
            scales = jnp.broadcast_to(scales, (GRAIN, GRAIN)).T
            block = words[u, g * words_per : (g + 1) * words_per, :]
            for k in range(BYTES):
                codes = jnp.right_shift(jnp.left_shift(block, 24 - 8 * k), 24).astype(jnp.float32)
                part = scales[k * words_per : (k + 1) * words_per]
                part = jnp.concatenate([part] * (block.shape[1] // GRAIN), axis=1)
                start = g * GRAIN + k * words_per
                out[u, start : start + words_per, :] = (codes * part).astype(jnp.bfloat16)


def history_rows(codes, scale_index, scale_table):
    users, words, width = codes.shape
    places = words * BYTES
    levels = scale_table.shape[0]
    return pl.pallas_call(
        history_body,
        grid=(users // BATCH,),
        in_specs=[
            pl.BlockSpec((BATCH, words, width), lambda u: (u, 0, 0)),
            pl.BlockSpec((users, places), lambda u: (0, 0)),
            pl.BlockSpec((1, levels), lambda u: (0, 0)),
        ],
        out_specs=pl.BlockSpec((BATCH, places, width), lambda u: (u, 0, 0)),
        out_shape=jax.ShapeDtypeStruct((users, places, width), jnp.bfloat16),
        cost_estimate=cost(2e9, 6e6),
        compiler_params=room(FULL),
        name="history",
    )(codes, scale_index, scale_table.reshape(1, levels))


def project_body(rows, key_w, value_wt, keys, values):
    width = key_w.shape[0]
    half = width // 2
    for u in range(rows.shape[0]):
        h = rows[u]
        keys[u] = dot(h, key_w[...]).astype(jnp.bfloat16)
        v = dot(value_wt[...], h, NT).astype(jnp.bfloat16)
        ones = jnp.ones((ONES, h.shape[0]), jnp.bfloat16)
        for p in range(2):
            at = p * (half + ONES)
            values[u, at : at + half, :] = v[p * half : (p + 1) * half]
            values[u, at + half : at + half + ONES, :] = ones


def project(rows, key_w, value_wt):
    users, places, width = rows.shape
    tall = width + 2 * ONES
    return pl.pallas_call(
        project_body,
        grid=(users // BATCH,),
        in_specs=[
            pl.BlockSpec((BATCH, places, width), lambda u: (u, 0, 0)),
            pl.BlockSpec((width, width), lambda u: (0, 0)),
            pl.BlockSpec((width, width), lambda u: (0, 0)),
        ],
        out_specs=[
            pl.BlockSpec((BATCH, places, width), lambda u: (u, 0, 0)),
            pl.BlockSpec((BATCH, tall, places), lambda u: (u, 0, 0)),
        ],
        out_shape=[
            jax.ShapeDtypeStruct((users, places, width), jnp.bfloat16),
            jax.ShapeDtypeStruct((users, tall, places), jnp.bfloat16),
        ],
        cost_estimate=cost(3e9, 12e6),
        compiler_params=room(12),
        name="project",
    )(rows, key_w, value_wt)


def query_body(rows, weight, out):
    head = weight.shape[1] // HEADS
    q = dot(rows[...], weight[...]).astype(jnp.bfloat16)
    out[...] = q * jnp.bfloat16(head**-0.5)


def query_rows(rows, weight):
    return pl.pallas_call(
        query_body,
        out_shape=jax.ShapeDtypeStruct((rows.shape[0], weight.shape[1]), jnp.bfloat16),
        cost_estimate=cost(3e7, 4e5),
        compiler_params=room(2),
        name="query",
    )(rows, weight)


def parts_of(peak):
    hi = peak.astype(jnp.bfloat16).astype(jnp.float32)
    mid = (peak - hi).astype(jnp.bfloat16).astype(jnp.float32)
    return [hi, mid, peak - hi - mid]


def pair_query(q, p):
    pair = 2 * q.shape[1] // HEADS
    lane = lax.broadcasted_iota(jnp.int32, (q.shape[0], pair), 1)
    both = q[:, p * pair : (p + 1) * pair].astype(jnp.float32)
    two = [jnp.where(lane < pair // 2, both, 0.0), jnp.where(lane < pair // 2, 0.0, both)]
    return jnp.concatenate(two, axis=0).astype(jnp.bfloat16)


def score_pair(p, k, q, counts, sources, scores):
    per = sources[0].shape[1] // GRAIN
    pair = 2 * q.shape[1] // HEADS
    right = pair_query(q, p)
    tops = []
    for half, source in enumerate(sources):
        for t in range(per):
            s = dot(source[k, t * GRAIN : (t + 1) * GRAIN, p * pair : (p + 1) * pair], right, NT)
            at = (half * per + t) * GRAIN
            scores[at : at + GRAIN, :] = s
            tops.append(jnp.where(t < counts[half], jnp.max(s, axis=0, keepdims=True), NEG))
    return functools.reduce(jnp.maximum, tops)


def blend_pair(p, k, peak, counts, sources, scores, weights):
    span = sources[0].shape[2]
    per = span // GRAIN
    tall = sources[0].shape[1] // (HEADS // 2)
    o = 0.0
    for half, source in enumerate(sources):
        for t in range(per):
            lift = jnp.where(t < counts[half], peak, -NEG)
            rows = slice((half * per + t) * GRAIN, (half * per + t + 1) * GRAIN)
            weights[rows, :] = jnp.exp(scores[rows, :] - lift).astype(jnp.bfloat16)
        o = o + dot(source[k, p * tall : (p + 1) * tall, :], weights[half * span : (half + 1) * span, :])
    return o


def attend_body(base, live, *refs):
    hops, refs = refs[: 2 * SPAN + 2], refs[2 * SPAN + 2 :]
    (k_own, k_other, v_own, v_other, order), refs = refs[:5], refs[5:]
    outs, (scores, weights, held) = refs[:SPAN], refs[SPAN:]
    lanes = held.shape[1] // GROUP
    batch, _, width = k_own.shape
    pair = 2 * width // HEADS
    head = pair // 2
    pairs = HEADS // 2
    i = pl.program_id(1)
    north = live[2, 0] > 0

    def begin(n):
        k, p = divmod(n, pairs)
        place = pl.program_id(0) * GROUP + i * batch + k
        user = base + place
        counts = (live[0, user], live[1, user])
        rows = [jnp.where(north, hops[j + 2][user], hops[j][user]) for j in range(2 * SPAN)]
        q = jnp.concatenate(rows, axis=0)
        return counts, score_pair(p, k, q, counts, (k_own, k_other), scores.at[n])

    def end(n, counts, peak):
        k, p = divmod(n, pairs)
        at = pl.ds(pl.multiple_of((i * batch + k) * lanes, lanes), lanes)
        o = blend_pair(p, k, peak, counts, (v_own, v_other), scores.at[n], weights.at[n])
        held[p * pair : p * pair + head, at] = o[0:head, 0:lanes].astype(jnp.bfloat16)
        held[p * pair + head : (p + 1) * pair, at] = o[head:pair, lanes:].astype(jnp.bfloat16)
        return [o[pair : pair + 1, 0:lanes], o[pair : pair + 1, lanes:]]

    begun = [begin(0)]
    totals = []
    for n in range(batch * pairs):
        if n + 1 < batch * pairs:
            begun.append(begin(n + 1))
        totals.append(end(n, *begun[n]))
    for k in range(batch):
        at = pl.ds(pl.multiple_of((i * batch + k) * lanes, lanes), lanes)
        peaks = [begun[k * pairs + p][1] for p in range(pairs)]
        peak = jnp.concatenate([x for p in peaks for x in (p[:, 0:lanes], p[:, lanes:])], axis=0)
        sums = [x for p in range(pairs) for x in totals[k * pairs + p]]
        held[width : width + STATS, at] = jnp.concatenate(parts_of(peak) + sums, axis=0).astype(jnp.bfloat16)

    @pl.when(i == GROUP // batch - 1)
    def _():
        mixed = dot(held[...], order[...]).astype(jnp.bfloat16)
        for s in range(SPAN):
            outs[s][...] = mixed[:, s * lanes : (s + 1) * lanes]


def attend(base, groups, live, hops, k_own, k_other, v_own, v_other, order):
    cand, width = hops[0].shape[1:]
    places = k_own.shape[1]
    tall = v_own.shape[1]
    lanes = cand * 2 * SPAN
    deep = width + STATS
    batch = 2
    some = lambda g, i, live: (base // batch + g * (GROUP // batch) + i, 0, 0)
    return pl.pallas_call(
        functools.partial(attend_body, base),
        grid_spec=pltpu.PrefetchScalarGridSpec(
            num_scalar_prefetch=1,
            grid=(groups, GROUP // batch),
            in_specs=[pl.BlockSpec(memory_space=pltpu.VMEM) for _ in hops]
            + [
                pl.BlockSpec((batch, places, width), some),
                pl.BlockSpec((batch, places, width), some),
                pl.BlockSpec((batch, tall, places), some),
                pl.BlockSpec((batch, tall, places), some),
                pl.BlockSpec(memory_space=pltpu.VMEM),
            ],
            out_specs=[pl.BlockSpec((deep, lanes), lambda g, i, live: (0, g))] * SPAN,
            scratch_shapes=[
                pltpu.VMEM((batch * HEADS // 2, 2 * places, 2 * lanes), jnp.float32),
                pltpu.VMEM((batch * HEADS // 2, 2 * places, 2 * lanes), jnp.bfloat16),
                pltpu.VMEM((deep, GROUP * lanes), jnp.bfloat16),
            ],
        ),
        out_shape=[jax.ShapeDtypeStruct((deep, groups * lanes), jnp.bfloat16)] * SPAN,
        cost_estimate=cost(3e9 * groups, 5e6),
        compiler_params=room(20),
        name="attend",
    )(live, *hops, k_own, k_other, v_own, v_other, order)


def merged(a, b):
    width = a.shape[0] - STATS
    head = width // HEADS
    sa, sb = a[width:].astype(jnp.float32), b[width:].astype(jnp.float32)
    pa = sa[0:4] + sa[4:8] + sa[8:12]
    pb = sb[0:4] + sb[4:8] + sb[8:12]
    peak = jnp.maximum(pa, pb)
    fa, fb = jnp.exp(pa - peak), jnp.exp(pb - peak)
    total = fa * sa[12:16] + fb * sb[12:16]
    rows = []
    for h in range(HEADS):
        na = a[h * head : (h + 1) * head].astype(jnp.float32)
        nb = b[h * head : (h + 1) * head].astype(jnp.float32)
        rows.append(na * fa[h : h + 1] + nb * fb[h : h + 1])
    return rows, peak, total


def packed(rows, peak, total):
    stats = jnp.concatenate(parts_of(peak) + [total], axis=0)
    return jnp.concatenate([r.astype(jnp.bfloat16) for r in rows] + [stats.astype(jnp.bfloat16)], axis=0)


def merge_body(came, *refs):
    mine, out = refs[:-1], refs[-1]
    lanes = came.shape[1] // len(mine)
    for n, m in enumerate(mine):
        at = slice(n * lanes, (n + 1) * lanes)
        out[:, at] = packed(*merged(came[:, at], m[...]))


def merge(came, mine):
    return pl.pallas_call(
        merge_body,
        out_shape=jax.ShapeDtypeStruct(came.shape, jnp.bfloat16),
        cost_estimate=cost(1e8, 5e5),
        compiler_params=room(3),
        name="merge",
    )(came, *mine)


def split_body(parts, *refs):
    came, mine, (order, near, far) = refs[:parts], refs[parts:-3], refs[-3:]
    lanes = order.shape[0]
    per = len(mine) // parts
    for n, m in enumerate(mine):
        at = (n % per) * lanes
        both = packed(*merged(came[n // per][:, at : at + lanes], m[...]))
        both = dot(both, order[...]).astype(jnp.bfloat16)
        to = slice(n * lanes // 2, (n + 1) * lanes // 2)
        near[:, to] = both[:, : lanes // 2]
        far[:, to] = both[:, lanes // 2 :]


def split(came, mine, order):
    deep, lanes = came[0].shape
    shape = jax.ShapeDtypeStruct((deep, lanes * len(came) // 2), jnp.bfloat16)
    return pl.pallas_call(
        functools.partial(split_body, len(came)),
        out_shape=[shape] * 2,
        cost_estimate=cost(1e8, 1e6),
        compiler_params=room(6),
        name="split",
    )(*came, *mine, order)


def finish_body(a, b, out_w, gain, hidden_w, bias, score_w, interest, logits):
    rows, _, total = merged(a[...], b[...])
    attended = jnp.concatenate(
        [(r / total[h : h + 1]).astype(jnp.bfloat16) for h, r in enumerate(rows)], axis=0
    )
    found = dot(attended, out_w[...], TN).astype(jnp.bfloat16)
    interest[...] = found
    f = found.astype(jnp.float32)
    normed = f * lax.rsqrt(jnp.mean(f * f, axis=1, keepdims=True) + 1e-6) * gain[...]
    v = dot(normed.astype(jnp.bfloat16), hidden_w[...]) + bias[...]
    hidden = (v / (1.0 + jnp.exp(-v))).astype(jnp.bfloat16)
    row = dot(jnp.broadcast_to(score_w[...], (16, v.shape[1])), hidden, NT)[0:1]
    users, cand = logits.shape
    lane = lax.broadcasted_iota(jnp.int32, (users, users * cand), 1)
    mine = lane // cand == lax.broadcasted_iota(jnp.int32, (users, users * cand), 0)
    fold = lax.broadcasted_iota(jnp.int32, (users * cand, cand), 0) % cand
    fold = (fold == lax.broadcasted_iota(jnp.int32, (users * cand, cand), 1)).astype(jnp.bfloat16)
    folded = [dot(jnp.where(mine, r, 0.0).astype(jnp.bfloat16), fold) for r in parts_of(row)]
    logits[...] = folded[0] + folded[1] + folded[2]


def finish(users, a, b, out_w, gain, hidden_w, bias, score_w):
    width, wide = hidden_w.shape
    lanes = a.shape[1]
    return pl.pallas_call(
        finish_body,
        out_shape=[
            jax.ShapeDtypeStruct((lanes, width), jnp.bfloat16),
            jax.ShapeDtypeStruct((users, lanes // users), jnp.float32),
        ],
        cost_estimate=cost(2e8, 1e6),
        compiler_params=room(8),
        name="finish",
    )(a, b, out_w, gain.reshape(1, width), hidden_w, bias.reshape(1, wide), score_w.reshape(1, wide))


def reorder(shape, axes):
    size = 1
    for n in shape:
        size *= n
    spot = lax.broadcasted_iota(jnp.int32, (size, size), 1)
    dims = [shape[a] for a in axes]
    digits = []
    for n in reversed(dims):
        digits.insert(0, spot % n)
        spot = spot // n
    source = 0
    for a, n in enumerate(shape):
        source = source * n + digits[axes.index(a)]
    return (lax.broadcasted_iota(jnp.int32, (size, size), 0) == source).astype(jnp.bfloat16)


def solution(mesh):
    peers = mesh.shape["seq"]
    chips = peers // 2
    slots = chips // 2
    near = lambda d, c: (d % chips) * 2 + c
    ring = [(near(d, 0), near(d + 1, 0)) for d in range(chips)] + [(near(d, 1), near(d - 1, 1)) for d in range(chips)]
    stay = [(near(d, 0), near(d, 0)) for d in range(chips)] + [(near(d, 1), near(d - 1, 1)) for d in range(chips)]
    cross = [(near(d, 1), near(d, 0)) for d in range(chips)] + [(near(d, 0), near(d - 1, 1)) for d in range(chips)]
    swap = [(near(d, c), near(d, 1 - c)) for d in range(chips) for c in range(2)]
    back = lambda pairs: [(b, a) for a, b in pairs]

    def on_device(
        candidates,
        codes,
        scale_index,
        lengths,
        scale_table,
        query_weight,
        key_weight,
        value_weight,
        out_weight,
        norm_gain,
        hidden_weight,
        hidden_bias,
        score_weight,
    ):
        users, cand, width = candidates.shape
        places = scale_index.shape[1]
        send = lambda array, pairs: lax.ppermute(array, "seq", pairs)
        me = lax.axis_index("seq")
        mate = me + 1 - 2 * (me % 2)
        starts = jnp.stack([me, mate])[:, None] * places
        live = jnp.clip((lengths[None, :] - starts) // GRAIN, 0, places // GRAIN).astype(jnp.int32)
        live = jnp.concatenate([live, jnp.full((1, users), me % 2, jnp.int32)])

        mine = query_rows(candidates.reshape(users * cand, width), query_weight).reshape(users, cand, width)
        hops = [mine, send(mine, swap)]
        for _ in range(1, slots + 1):
            for _ in range(2):
                hops.append(send(hops[-2], ring))

        value_wt = value_weight.T
        own = history_rows(codes, scale_index, scale_table)
        other = send(own, swap)
        k_own, v_own = project(own, key_weight, value_wt)
        k_other, v_other = project(other, key_weight, value_wt)

        order = reorder((GROUP, SPAN, 2 * cand), (1, 0, 2))
        partial = []
        for block, groups in ((0, 1), (1, users // PARTS // GROUP)):
            calls = []
            for call in range(users // (groups * GROUP)):
                base = call * groups * GROUP
                near_hops = hops[2 * block * SPAN : 2 * (block + 1) * SPAN + 2]
                calls.append(attend(base, groups, live, near_hops, k_own, k_other, v_own, v_other, order))
            partial.append(calls)

        def result(part, slot):
            calls = partial[slot // SPAN]
            per = len(calls) // PARTS
            return [c[slot % SPAN] for c in calls[part * per : (part + 1) * per]]

        come = [result(part, slots - 1)[0] for part in range(PARTS)]
        for slot in range(slots - 2, -1, -1):
            come = [send(c, back(ring)) for c in come]
            if slot:
                come = [merge(c, result(part, slot)) for part, c in enumerate(come)]
        halves = reorder((GROUP, 2, cand), (1, 0, 2))
        first, second = split(come, [x for part in range(PARTS) for x in result(part, 0)], halves)
        first, second = send(first, back(stay)), send(second, back(cross))
        interest, logits = finish(
            users, first, second, out_weight, norm_gain, hidden_weight, hidden_bias, score_weight
        )
        return interest.reshape(users, cand, width), logits

    in_specs = (
        P("groups", "seq", None),
        P("groups", "seq", None),
        P("groups", "seq"),
        P("groups"),
    ) + (P(),) * 9
    out_specs = (P("groups", "seq", None), P("groups", "seq"))

    return jax.shard_map(on_device, mesh=mesh, in_specs=in_specs, out_specs=out_specs, check_vma=False)
```

```python
import functools

import jax
import jax.numpy as jnp
from jax import lax
from jax.experimental import pallas as pl
from jax.experimental.pallas import tpu as pltpu
from jax.sharding import PartitionSpec as P


HEADS = 4
GRAIN = 128
BYTES = 4
NEG = -1e30
SPAN = 4
GROUP = 4
STATS = 16
ONES = 16
PARTS = 2
BATCH = 4
FULL = 62.5

NT = (((1,), (1,)), ((), ()))
TN = (((0,), (0,)), ((), ()))


def dot(a, b, dims=(((1,), (0,)), ((), ()))):
    return lax.dot_general(a, b, dims, preferred_element_type=jnp.float32)


def cost(flops, moved):
    return pl.CostEstimate(flops=int(flops), bytes_accessed=int(moved), transcendentals=0)


def room(mib):
    return pltpu.CompilerParams(vmem_limit_bytes=int(mib * 2**20))


def history_body(words, index, table, out):
    levels = table.shape[1]
    words_per = GRAIN // BYTES
    spot = lax.broadcasted_iota(jnp.int32, (GRAIN, GRAIN), 0)
    place = lax.broadcasted_iota(jnp.int32, (GRAIN, GRAIN), 1)
    moves = (spot == BYTES * (place % words_per) + place // words_per).astype(jnp.bfloat16)
    level = lax.broadcasted_iota(jnp.int32, (levels, GRAIN), 0).astype(jnp.float32)
    entry = jnp.broadcast_to(table[...], (GRAIN, levels)).T
    users = words.shape[0]
    first = pl.program_id(0) * users
    for u in range(users):
        indices = index[pl.ds(first + u, 1), :].astype(jnp.float32)
        for g in range(words.shape[1] // words_per):
            row = indices[:, g * GRAIN : (g + 1) * GRAIN]
            row = jnp.broadcast_to(row, (16, GRAIN)).astype(jnp.bfloat16)
            row = dot(row, moves)[0:1]
            scales = jnp.sum(jnp.where(level == row, entry, 0.0), axis=0, keepdims=True)
            scales = jnp.broadcast_to(scales, (GRAIN, GRAIN)).T
            block = words[u, g * words_per : (g + 1) * words_per, :]
            for k in range(BYTES):
                codes = jnp.right_shift(jnp.left_shift(block, 24 - 8 * k), 24).astype(jnp.float32)
                part = scales[k * words_per : (k + 1) * words_per]
                part = jnp.concatenate([part] * (block.shape[1] // GRAIN), axis=1)
                start = g * GRAIN + k * words_per
                out[u, start : start + words_per, :] = (codes * part).astype(jnp.bfloat16)


def history_rows(codes, scale_index, scale_table):
    users, words, width = codes.shape
    places = words * BYTES
    levels = scale_table.shape[0]
    return pl.pallas_call(
        history_body,
        grid=(users // BATCH,),
        in_specs=[
            pl.BlockSpec((BATCH, words, width), lambda u: (u, 0, 0)),
            pl.BlockSpec((users, places), lambda u: (0, 0)),
            pl.BlockSpec((1, levels), lambda u: (0, 0)),
        ],
        out_specs=pl.BlockSpec((BATCH, places, width), lambda u: (u, 0, 0)),
        out_shape=jax.ShapeDtypeStruct((users, places, width), jnp.bfloat16),
        cost_estimate=cost(2e9, 6e6),
        compiler_params=room(FULL),
        name="history",
    )(codes, scale_index, scale_table.reshape(1, levels))


def project_body(rows, key_w, value_wt, keys, values):
    width = key_w.shape[0]
    half = width // 2
    for u in range(rows.shape[0]):
        h = rows[u]
        keys[u] = dot(h, key_w[...]).astype(jnp.bfloat16)
        v = dot(value_wt[...], h, NT).astype(jnp.bfloat16)
        ones = jnp.ones((ONES, h.shape[0]), jnp.bfloat16)
        for p in range(2):
            at = p * (half + ONES)
            values[u, at : at + half, :] = v[p * half : (p + 1) * half]
            values[u, at + half : at + half + ONES, :] = ones


def project(rows, key_w, value_wt):
    users, places, width = rows.shape
    tall = width + 2 * ONES
    return pl.pallas_call(
        project_body,
        grid=(users // BATCH,),
        in_specs=[
            pl.BlockSpec((BATCH, places, width), lambda u: (u, 0, 0)),
            pl.BlockSpec((width, width), lambda u: (0, 0)),
            pl.BlockSpec((width, width), lambda u: (0, 0)),
        ],
        out_specs=[
            pl.BlockSpec((BATCH, places, width), lambda u: (u, 0, 0)),
            pl.BlockSpec((BATCH, tall, places), lambda u: (u, 0, 0)),
        ],
        out_shape=[
            jax.ShapeDtypeStruct((users, places, width), jnp.bfloat16),
            jax.ShapeDtypeStruct((users, tall, places), jnp.bfloat16),
        ],
        cost_estimate=cost(3e9, 12e6),
        compiler_params=room(12),
        name="project",
    )(rows, key_w, value_wt)


def query_body(rows, weight, out):
    head = weight.shape[1] // HEADS
    q = dot(rows[...], weight[...]).astype(jnp.bfloat16)
    out[...] = q * jnp.bfloat16(head**-0.5)


def query_rows(rows, weight):
    return pl.pallas_call(
        query_body,
        out_shape=jax.ShapeDtypeStruct((rows.shape[0], weight.shape[1]), jnp.bfloat16),
        cost_estimate=cost(3e7, 4e5),
        compiler_params=room(2),
        name="query",
    )(rows, weight)


def parts_of(peak):
    hi = peak.astype(jnp.bfloat16).astype(jnp.float32)
    mid = (peak - hi).astype(jnp.bfloat16).astype(jnp.float32)
    return [hi, mid, peak - hi - mid]


def pair_query(q, p):
    pair = 2 * q.shape[1] // HEADS
    lane = lax.broadcasted_iota(jnp.int32, (q.shape[0], pair), 1)
    both = q[:, p * pair : (p + 1) * pair].astype(jnp.float32)
    two = [jnp.where(lane < pair // 2, both, 0.0), jnp.where(lane < pair // 2, 0.0, both)]
    return jnp.concatenate(two, axis=0).astype(jnp.bfloat16)


def score_pair(p, k, q, counts, sources, scores):
    per = sources[0].shape[1] // GRAIN
    pair = 2 * q.shape[1] // HEADS
    right = pair_query(q, p)
    tops = []
    for half, source in enumerate(sources):
        for t in range(per):
            s = dot(source[k, t * GRAIN : (t + 1) * GRAIN, p * pair : (p + 1) * pair], right, NT)
            at = (half * per + t) * GRAIN
            scores[at : at + GRAIN, :] = s
            tops.append(jnp.where(t < counts[half], jnp.max(s, axis=0, keepdims=True), NEG))
    return functools.reduce(jnp.maximum, tops)


def blend_pair(p, k, peak, counts, sources, scores, weights):
    span = sources[0].shape[2]
    per = span // GRAIN
    tall = sources[0].shape[1] // (HEADS // 2)
    o = 0.0
    for half, source in enumerate(sources):
        for t in range(per):
            lift = jnp.where(t < counts[half], peak, -NEG)
            rows = slice((half * per + t) * GRAIN, (half * per + t + 1) * GRAIN)
            weights[rows, :] = jnp.exp(scores[rows, :] - lift).astype(jnp.bfloat16)
        o = o + dot(source[k, p * tall : (p + 1) * tall, :], weights[half * span : (half + 1) * span, :])
    return o


def attend_body(base, live, *refs):
    hops, refs = refs[: 2 * SPAN + 2], refs[2 * SPAN + 2 :]
    (k_own, k_other, v_own, v_other, order), refs = refs[:5], refs[5:]
    outs, (scores, weights, held) = refs[:SPAN], refs[SPAN:]
    lanes = held.shape[1] // GROUP
    batch, _, width = k_own.shape
    pair = 2 * width // HEADS
    head = pair // 2
    pairs = HEADS // 2
    i = pl.program_id(1)
    north = live[2, 0] > 0

    def begin(n):
        k, p = divmod(n, pairs)
        place = pl.program_id(0) * GROUP + i * batch + k
        user = base + place
        counts = (live[0, user], live[1, user])
        rows = [jnp.where(north, hops[j + 2][user], hops[j][user]) for j in range(2 * SPAN)]
        q = jnp.concatenate(rows, axis=0)
        return counts, score_pair(p, k, q, counts, (k_own, k_other), scores.at[n])

    def end(n, counts, peak):
        k, p = divmod(n, pairs)
        at = pl.ds(pl.multiple_of((i * batch + k) * lanes, lanes), lanes)
        o = blend_pair(p, k, peak, counts, (v_own, v_other), scores.at[n], weights.at[n])
        held[p * pair : p * pair + head, at] = o[0:head, 0:lanes].astype(jnp.bfloat16)
        held[p * pair + head : (p + 1) * pair, at] = o[head:pair, lanes:].astype(jnp.bfloat16)
        return [o[pair : pair + 1, 0:lanes], o[pair : pair + 1, lanes:]]

    begun = [begin(0)]
    totals = []
    for n in range(batch * pairs):
        if n + 1 < batch * pairs:
            begun.append(begin(n + 1))
        totals.append(end(n, *begun[n]))
    for k in range(batch):
        at = pl.ds(pl.multiple_of((i * batch + k) * lanes, lanes), lanes)
        peaks = [begun[k * pairs + p][1] for p in range(pairs)]
        peak = jnp.concatenate([x for p in peaks for x in (p[:, 0:lanes], p[:, lanes:])], axis=0)
        sums = [x for p in range(pairs) for x in totals[k * pairs + p]]
        held[width : width + STATS, at] = jnp.concatenate(parts_of(peak) + sums, axis=0).astype(jnp.bfloat16)

    @pl.when(i == GROUP // batch - 1)
    def _():
        mixed = dot(held[...], order[...]).astype(jnp.bfloat16)
        for s in range(SPAN):
            outs[s][...] = mixed[:, s * lanes : (s + 1) * lanes]


def attend(base, groups, live, hops, k_own, k_other, v_own, v_other, order):
    cand, width = hops[0].shape[1:]
    places = k_own.shape[1]
    tall = v_own.shape[1]
    lanes = cand * 2 * SPAN
    deep = width + STATS
    batch = 2
    some = lambda g, i, live: (base // batch + g * (GROUP // batch) + i, 0, 0)
    return pl.pallas_call(
        functools.partial(attend_body, base),
        grid_spec=pltpu.PrefetchScalarGridSpec(
            num_scalar_prefetch=1,
            grid=(groups, GROUP // batch),
            in_specs=[pl.BlockSpec(memory_space=pltpu.VMEM) for _ in hops]
            + [
                pl.BlockSpec((batch, places, width), some),
                pl.BlockSpec((batch, places, width), some),
                pl.BlockSpec((batch, tall, places), some),
                pl.BlockSpec((batch, tall, places), some),
                pl.BlockSpec(memory_space=pltpu.VMEM),
            ],
            out_specs=[pl.BlockSpec((deep, lanes), lambda g, i, live: (0, g))] * SPAN,
            scratch_shapes=[
                pltpu.VMEM((batch * HEADS // 2, 2 * places, 2 * lanes), jnp.float32),
                pltpu.VMEM((batch * HEADS // 2, 2 * places, 2 * lanes), jnp.bfloat16),
                pltpu.VMEM((deep, GROUP * lanes), jnp.bfloat16),
            ],
        ),
        out_shape=[jax.ShapeDtypeStruct((deep, groups * lanes), jnp.bfloat16)] * SPAN,
        cost_estimate=cost(3e9 * groups, 5e6),
        compiler_params=room(20),
        name="attend",
    )(live, *hops, k_own, k_other, v_own, v_other, order)


def merged(a, b):
    width = a.shape[0] - STATS
    head = width // HEADS
    sa, sb = a[width:].astype(jnp.float32), b[width:].astype(jnp.float32)
    pa = sa[0:4] + sa[4:8] + sa[8:12]
    pb = sb[0:4] + sb[4:8] + sb[8:12]
    peak = jnp.maximum(pa, pb)
    fa, fb = jnp.exp(pa - peak), jnp.exp(pb - peak)
    total = fa * sa[12:16] + fb * sb[12:16]
    rows = []
    for h in range(HEADS):
        na = a[h * head : (h + 1) * head].astype(jnp.float32)
        nb = b[h * head : (h + 1) * head].astype(jnp.float32)
        rows.append(na * fa[h : h + 1] + nb * fb[h : h + 1])
    return rows, peak, total


def packed(rows, peak, total):
    stats = jnp.concatenate(parts_of(peak) + [total], axis=0)
    return jnp.concatenate([r.astype(jnp.bfloat16) for r in rows] + [stats.astype(jnp.bfloat16)], axis=0)


def merge_body(came, *refs):
    mine, out = refs[:-1], refs[-1]
    lanes = came.shape[1] // len(mine)
    for n, m in enumerate(mine):
        at = slice(n * lanes, (n + 1) * lanes)
        out[:, at] = packed(*merged(came[:, at], m[...]))


def merge(came, mine):
    return pl.pallas_call(
        merge_body,
        out_shape=jax.ShapeDtypeStruct(came.shape, jnp.bfloat16),
        cost_estimate=cost(1e8, 5e5),
        compiler_params=room(3),
        name="merge",
    )(came, *mine)


def split_body(parts, *refs):
    came, mine, (order, near, far) = refs[:parts], refs[parts:-3], refs[-3:]
    lanes = order.shape[0]
    per = len(mine) // parts
    for n, m in enumerate(mine):
        at = (n % per) * lanes
        both = packed(*merged(came[n // per][:, at : at + lanes], m[...]))
        both = dot(both, order[...]).astype(jnp.bfloat16)
        to = slice(n * lanes // 2, (n + 1) * lanes // 2)
        near[:, to] = both[:, : lanes // 2]
        far[:, to] = both[:, lanes // 2 :]


def split(came, mine, order):
    deep, lanes = came[0].shape
    shape = jax.ShapeDtypeStruct((deep, lanes * len(came) // 2), jnp.bfloat16)
    return pl.pallas_call(
        functools.partial(split_body, len(came)),
        out_shape=[shape] * 2,
        cost_estimate=cost(1e8, 1e6),
        compiler_params=room(6),
        name="split",
    )(*came, *mine, order)


def finish_body(a, b, out_w, gain, hidden_w, bias, score_w, interest, logits):
    rows, _, total = merged(a[...], b[...])
    attended = jnp.concatenate(
        [(r / total[h : h + 1]).astype(jnp.bfloat16) for h, r in enumerate(rows)], axis=0
    )
    found = dot(attended, out_w[...], TN).astype(jnp.bfloat16)
    interest[...] = found
    f = found.astype(jnp.float32)
    normed = f * lax.rsqrt(jnp.mean(f * f, axis=1, keepdims=True) + 1e-6) * gain[...]
    v = dot(normed.astype(jnp.bfloat16), hidden_w[...]) + bias[...]
    hidden = (v / (1.0 + jnp.exp(-v))).astype(jnp.bfloat16)
    row = dot(jnp.broadcast_to(score_w[...], (16, v.shape[1])), hidden, NT)[0:1]
    users, cand = logits.shape
    lane = lax.broadcasted_iota(jnp.int32, (users, users * cand), 1)
    mine = lane // cand == lax.broadcasted_iota(jnp.int32, (users, users * cand), 0)
    fold = lax.broadcasted_iota(jnp.int32, (users * cand, cand), 0) % cand
    fold = (fold == lax.broadcasted_iota(jnp.int32, (users * cand, cand), 1)).astype(jnp.bfloat16)
    folded = [dot(jnp.where(mine, r, 0.0).astype(jnp.bfloat16), fold) for r in parts_of(row)]
    logits[...] = folded[0] + folded[1] + folded[2]


def finish(users, a, b, out_w, gain, hidden_w, bias, score_w):
    width, wide = hidden_w.shape
    lanes = a.shape[1]
    return pl.pallas_call(
        finish_body,
        out_shape=[
            jax.ShapeDtypeStruct((lanes, width), jnp.bfloat16),
            jax.ShapeDtypeStruct((users, lanes // users), jnp.float32),
        ],
        cost_estimate=cost(2e8, 1e6),
        compiler_params=room(8),
        name="finish",
    )(a, b, out_w, gain.reshape(1, width), hidden_w, bias.reshape(1, wide), score_w.reshape(1, wide))


def reorder(shape, axes):
    size = 1
    for n in shape:
        size *= n
    spot = lax.broadcasted_iota(jnp.int32, (size, size), 1)
    dims = [shape[a] for a in axes]
    digits = []
    for n in reversed(dims):
        digits.insert(0, spot % n)
        spot = spot // n
    source = 0
    for a, n in enumerate(shape):
        source = source * n + digits[axes.index(a)]
    return (lax.broadcasted_iota(jnp.int32, (size, size), 0) == source).astype(jnp.bfloat16)


def solution(mesh):
    peers = mesh.shape["seq"]
    chips = peers // 2
    slots = chips // 2
    near = lambda d, c: (d % chips) * 2 + c
    ring = [(near(d, 0), near(d + 1, 0)) for d in range(chips)] + [(near(d, 1), near(d - 1, 1)) for d in range(chips)]
    stay = [(near(d, 0), near(d, 0)) for d in range(chips)] + [(near(d, 1), near(d - 1, 1)) for d in range(chips)]
    cross = [(near(d, 1), near(d, 0)) for d in range(chips)] + [(near(d, 0), near(d - 1, 1)) for d in range(chips)]
    tail = [(near(d, 1), near(d - 1, 1)) for d in range(chips)]
    swap = [(near(d, c), near(d, 1 - c)) for d in range(chips) for c in range(2)]
    back = lambda pairs: [(b, a) for a, b in pairs]

    def on_device(
        candidates,
        codes,
        scale_index,
        lengths,
        scale_table,
        query_weight,
        key_weight,
        value_weight,
        out_weight,
        norm_gain,
        hidden_weight,
        hidden_bias,
        score_weight,
    ):
        users, cand, width = candidates.shape
        places = scale_index.shape[1]
        send = lambda array, pairs: lax.ppermute(array, "seq", pairs)
        me = lax.axis_index("seq")
        mate = me + 1 - 2 * (me % 2)
        starts = jnp.stack([me, mate])[:, None] * places
        live = jnp.clip((lengths[None, :] - starts) // GRAIN, 0, places // GRAIN).astype(jnp.int32)
        live = jnp.concatenate([live, jnp.full((1, users), me % 2, jnp.int32)])

        mine = query_rows(candidates.reshape(users * cand, width), query_weight).reshape(users, cand, width)
        hops = [mine, send(mine, swap)]
        for hop in range(1, slots + 1):
            for _ in range(2):
                hops.append(send(hops[-2], ring if hop < slots else tail))

        value_wt = value_weight.T
        own = history_rows(codes, scale_index, scale_table)
        other = send(own, swap)
        k_own, v_own = project(own, key_weight, value_wt)
        k_other, v_other = project(other, key_weight, value_wt)

        order = reorder((GROUP, SPAN, 2 * cand), (1, 0, 2))
        partial = []
        for block, groups in ((0, 1), (1, users // PARTS // GROUP)):
            calls = []
            for call in range(users // (groups * GROUP)):
                base = call * groups * GROUP
                near_hops = hops[2 * block * SPAN : 2 * (block + 1) * SPAN + 2]
                calls.append(attend(base, groups, live, near_hops, k_own, k_other, v_own, v_other, order))
            partial.append(calls)

        def result(part, slot):
            calls = partial[slot // SPAN]
            per = len(calls) // PARTS
            return [c[slot % SPAN] for c in calls[part * per : (part + 1) * per]]

        come = [result(part, slots - 1)[0] for part in range(PARTS)]
        for slot in range(slots - 2, -1, -1):
            come = [send(c, back(ring)) for c in come]
            if slot:
                come = [merge(c, result(part, slot)) for part, c in enumerate(come)]
        halves = reorder((GROUP, 2, cand), (1, 0, 2))
        first, second = split(come, [x for part in range(PARTS) for x in result(part, 0)], halves)
        first, second = send(first, back(stay)), send(second, back(cross))
        interest, logits = finish(
            users, first, second, out_weight, norm_gain, hidden_weight, hidden_bias, score_weight
        )
        return interest.reshape(users, cand, width), logits

    in_specs = (
        P("groups", "seq", None),
        P("groups", "seq", None),
        P("groups", "seq"),
        P("groups"),
    ) + (P(),) * 9
    out_specs = (P("groups", "seq", None), P("groups", "seq"))

    return jax.shard_map(on_device, mesh=mesh, in_specs=in_specs, out_specs=out_specs, check_vma=False)
```

```python
import functools

import jax
import jax.numpy as jnp
from jax import lax
from jax.experimental import pallas as pl
from jax.experimental.pallas import tpu as pltpu
from jax.sharding import PartitionSpec as P


HEADS = 4
GRAIN = 128
BYTES = 4
NEG = -1e30
SPAN = 4
GROUP = 4
STATS = 16
ONES = 16
PARTS = 2
BATCH = 4
FULL = 62.5

NT = (((1,), (1,)), ((), ()))
TN = (((0,), (0,)), ((), ()))


def dot(a, b, dims=(((1,), (0,)), ((), ()))):
    return lax.dot_general(a, b, dims, preferred_element_type=jnp.float32)


def cost(flops, moved):
    return pl.CostEstimate(flops=int(flops), bytes_accessed=int(moved), transcendentals=0)


def room(mib):
    return pltpu.CompilerParams(vmem_limit_bytes=int(mib * 2**20))


def history_body(words, index, table, out):
    levels = table.shape[1]
    words_per = GRAIN // BYTES
    spot = lax.broadcasted_iota(jnp.int32, (GRAIN, GRAIN), 0)
    place = lax.broadcasted_iota(jnp.int32, (GRAIN, GRAIN), 1)
    moves = (spot == BYTES * (place % words_per) + place // words_per).astype(jnp.bfloat16)
    level = lax.broadcasted_iota(jnp.int32, (levels, GRAIN), 0).astype(jnp.float32)
    entry = jnp.broadcast_to(table[...], (GRAIN, levels)).T
    users = words.shape[0]
    first = pl.program_id(0) * users
    for u in range(users):
        indices = index[pl.ds(first + u, 1), :].astype(jnp.float32)
        for g in range(words.shape[1] // words_per):
            row = indices[:, g * GRAIN : (g + 1) * GRAIN]
            row = jnp.broadcast_to(row, (16, GRAIN)).astype(jnp.bfloat16)
            row = dot(row, moves)[0:1]
            scales = jnp.sum(jnp.where(level == row, entry, 0.0), axis=0, keepdims=True)
            scales = jnp.broadcast_to(scales, (GRAIN, GRAIN)).T
            block = words[u, g * words_per : (g + 1) * words_per, :]
            for k in range(BYTES):
                codes = jnp.right_shift(jnp.left_shift(block, 24 - 8 * k), 24).astype(jnp.float32)
                part = scales[k * words_per : (k + 1) * words_per]
                part = jnp.concatenate([part] * (block.shape[1] // GRAIN), axis=1)
                start = g * GRAIN + k * words_per
                out[u, start : start + words_per, :] = (codes * part).astype(jnp.bfloat16)


def history_rows(codes, scale_index, scale_table):
    users, words, width = codes.shape
    places = words * BYTES
    levels = scale_table.shape[0]
    return pl.pallas_call(
        history_body,
        grid=(users // BATCH,),
        in_specs=[
            pl.BlockSpec((BATCH, words, width), lambda u: (u, 0, 0)),
            pl.BlockSpec((users, places), lambda u: (0, 0)),
            pl.BlockSpec((1, levels), lambda u: (0, 0)),
        ],
        out_specs=pl.BlockSpec((BATCH, places, width), lambda u: (u, 0, 0)),
        out_shape=jax.ShapeDtypeStruct((users, places, width), jnp.bfloat16),
        cost_estimate=cost(2e9, 6e6),
        compiler_params=room(FULL),
        name="history",
    )(codes, scale_index, scale_table.reshape(1, levels))


def project_body(rows, key_w, value_wt, keys, values):
    width = key_w.shape[0]
    half = width // 2
    for u in range(rows.shape[0]):
        h = rows[u]
        keys[u] = dot(h, key_w[...]).astype(jnp.bfloat16)
        v = dot(value_wt[...], h, NT).astype(jnp.bfloat16)
        ones = jnp.ones((ONES, h.shape[0]), jnp.bfloat16)
        for p in range(2):
            at = p * (half + ONES)
            values[u, at : at + half, :] = v[p * half : (p + 1) * half]
            values[u, at + half : at + half + ONES, :] = ones


def project(rows, key_w, value_wt):
    users, places, width = rows.shape
    tall = width + 2 * ONES
    return pl.pallas_call(
        project_body,
        grid=(users // BATCH,),
        in_specs=[
            pl.BlockSpec((BATCH, places, width), lambda u: (u, 0, 0)),
            pl.BlockSpec((width, width), lambda u: (0, 0)),
            pl.BlockSpec((width, width), lambda u: (0, 0)),
        ],
        out_specs=[
            pl.BlockSpec((BATCH, places, width), lambda u: (u, 0, 0)),
            pl.BlockSpec((BATCH, tall, places), lambda u: (u, 0, 0)),
        ],
        out_shape=[
            jax.ShapeDtypeStruct((users, places, width), jnp.bfloat16),
            jax.ShapeDtypeStruct((users, tall, places), jnp.bfloat16),
        ],
        cost_estimate=cost(3e9, 12e6),
        compiler_params=room(12),
        name="project",
    )(rows, key_w, value_wt)


def query_body(rows, weight, out):
    head = weight.shape[1] // HEADS
    q = dot(rows[...], weight[...]).astype(jnp.bfloat16)
    out[...] = q * jnp.bfloat16(head**-0.5)


def query_rows(rows, weight):
    return pl.pallas_call(
        query_body,
        out_shape=jax.ShapeDtypeStruct((rows.shape[0], weight.shape[1]), jnp.bfloat16),
        cost_estimate=cost(3e7, 4e5),
        compiler_params=room(2),
        name="query",
    )(rows, weight)


def parts_of(peak):
    hi = peak.astype(jnp.bfloat16).astype(jnp.float32)
    mid = (peak - hi).astype(jnp.bfloat16).astype(jnp.float32)
    return [hi, mid, peak - hi - mid]


def pair_query(q, p):
    pair = 2 * q.shape[1] // HEADS
    lane = lax.broadcasted_iota(jnp.int32, (q.shape[0], pair), 1)
    both = q[:, p * pair : (p + 1) * pair].astype(jnp.float32)
    two = [jnp.where(lane < pair // 2, both, 0.0), jnp.where(lane < pair // 2, 0.0, both)]
    return jnp.concatenate(two, axis=0).astype(jnp.bfloat16)


def score_pair(p, k, q, counts, sources, scores):
    per = sources[0].shape[1] // GRAIN
    pair = 2 * q.shape[1] // HEADS
    right = pair_query(q, p)
    tops = []
    for half, source in enumerate(sources):
        for t in range(per):
            s = dot(source[k, t * GRAIN : (t + 1) * GRAIN, p * pair : (p + 1) * pair], right, NT)
            at = (half * per + t) * GRAIN
            scores[at : at + GRAIN, :] = s
            tops.append(jnp.where(t < counts[half], jnp.max(s, axis=0, keepdims=True), NEG))
    return functools.reduce(jnp.maximum, tops)


def blend_pair(p, k, peak, counts, sources, scores, weights):
    span = sources[0].shape[2]
    per = span // GRAIN
    tall = sources[0].shape[1] // (HEADS // 2)
    o = 0.0
    for half, source in enumerate(sources):
        for t in range(per):
            lift = jnp.where(t < counts[half], peak, -NEG)
            rows = slice((half * per + t) * GRAIN, (half * per + t + 1) * GRAIN)
            weights[rows, :] = jnp.exp(scores[rows, :] - lift).astype(jnp.bfloat16)
        o = o + dot(source[k, p * tall : (p + 1) * tall, :], weights[half * span : (half + 1) * span, :])
    return o


def attend_body(base, live, *refs):
    hops, refs = refs[: 2 * SPAN + 2], refs[2 * SPAN + 2 :]
    (k_own, k_other, v_own, v_other, order), refs = refs[:5], refs[5:]
    outs, (scores, weights, held) = refs[:SPAN], refs[SPAN:]
    lanes = held.shape[1] // GROUP
    batch, _, width = k_own.shape
    pair = 2 * width // HEADS
    head = pair // 2
    pairs = HEADS // 2
    i = pl.program_id(1)
    north = live[2, 0] > 0

    def begin(n):
        k, p = divmod(n, pairs)
        place = pl.program_id(0) * GROUP + i * batch + k
        user = base + place
        counts = (live[0, user], live[1, user])
        rows = [jnp.where(north, hops[j + 2][user], hops[j][user]) for j in range(2 * SPAN)]
        q = jnp.concatenate(rows, axis=0)
        return counts, score_pair(p, k, q, counts, (k_own, k_other), scores.at[n])

    def end(n, counts, peak):
        k, p = divmod(n, pairs)
        at = pl.ds(pl.multiple_of((i * batch + k) * lanes, lanes), lanes)
        o = blend_pair(p, k, peak, counts, (v_own, v_other), scores.at[n], weights.at[n])
        held[p * pair : p * pair + head, at] = o[0:head, 0:lanes].astype(jnp.bfloat16)
        held[p * pair + head : (p + 1) * pair, at] = o[head:pair, lanes:].astype(jnp.bfloat16)
        return [o[pair : pair + 1, 0:lanes], o[pair : pair + 1, lanes:]]

    begun = [begin(0)]
    totals = []
    for n in range(batch * pairs):
        if n + 1 < batch * pairs:
            begun.append(begin(n + 1))
        totals.append(end(n, *begun[n]))
    for k in range(batch):
        at = pl.ds(pl.multiple_of((i * batch + k) * lanes, lanes), lanes)
        peaks = [begun[k * pairs + p][1] for p in range(pairs)]
        peak = jnp.concatenate([x for p in peaks for x in (p[:, 0:lanes], p[:, lanes:])], axis=0)
        sums = [x for p in range(pairs) for x in totals[k * pairs + p]]
        held[width : width + STATS, at] = jnp.concatenate(parts_of(peak) + sums, axis=0).astype(jnp.bfloat16)

    @pl.when(i == GROUP // batch - 1)
    def _():
        mixed = dot(held[...], order[...]).astype(jnp.bfloat16)
        for s in range(SPAN):
            outs[s][...] = mixed[:, s * lanes : (s + 1) * lanes]


def attend(base, groups, live, hops, k_own, k_other, v_own, v_other, order):
    cand, width = hops[0].shape[1:]
    places = k_own.shape[1]
    tall = v_own.shape[1]
    lanes = cand * 2 * SPAN
    deep = width + STATS
    batch = 2
    some = lambda g, i, live: (base // batch + g * (GROUP // batch) + i, 0, 0)
    return pl.pallas_call(
        functools.partial(attend_body, base),
        grid_spec=pltpu.PrefetchScalarGridSpec(
            num_scalar_prefetch=1,
            grid=(groups, GROUP // batch),
            in_specs=[pl.BlockSpec(memory_space=pltpu.VMEM) for _ in hops]
            + [
                pl.BlockSpec((batch, places, width), some),
                pl.BlockSpec((batch, places, width), some),
                pl.BlockSpec((batch, tall, places), some),
                pl.BlockSpec((batch, tall, places), some),
                pl.BlockSpec(memory_space=pltpu.VMEM),
            ],
            out_specs=[pl.BlockSpec((deep, lanes), lambda g, i, live: (0, g))] * SPAN,
            scratch_shapes=[
                pltpu.VMEM((batch * HEADS // 2, 2 * places, 2 * lanes), jnp.float32),
                pltpu.VMEM((batch * HEADS // 2, 2 * places, 2 * lanes), jnp.bfloat16),
                pltpu.VMEM((deep, GROUP * lanes), jnp.bfloat16),
            ],
        ),
        out_shape=[jax.ShapeDtypeStruct((deep, groups * lanes), jnp.bfloat16)] * SPAN,
        cost_estimate=cost(3e9 * groups, 5e6),
        compiler_params=room(20),
        name="attend",
    )(live, *hops, k_own, k_other, v_own, v_other, order)


def merged(a, b):
    width = a.shape[0] - STATS
    head = width // HEADS
    sa, sb = a[width:].astype(jnp.float32), b[width:].astype(jnp.float32)
    pa = sa[0:4] + sa[4:8] + sa[8:12]
    pb = sb[0:4] + sb[4:8] + sb[8:12]
    peak = jnp.maximum(pa, pb)
    fa, fb = jnp.exp(pa - peak), jnp.exp(pb - peak)
    total = fa * sa[12:16] + fb * sb[12:16]
    rows = []
    for h in range(HEADS):
        na = a[h * head : (h + 1) * head].astype(jnp.float32)
        nb = b[h * head : (h + 1) * head].astype(jnp.float32)
        rows.append(na * fa[h : h + 1] + nb * fb[h : h + 1])
    return rows, peak, total


def packed(rows, peak, total):
    stats = jnp.concatenate(parts_of(peak) + [total], axis=0)
    return jnp.concatenate([r.astype(jnp.bfloat16) for r in rows] + [stats.astype(jnp.bfloat16)], axis=0)


def merge_body(came, *refs):
    mine, out = refs[:-1], refs[-1]
    lanes = came.shape[1] // len(mine)
    for n, m in enumerate(mine):
        at = slice(n * lanes, (n + 1) * lanes)
        out[:, at] = packed(*merged(came[:, at], m[...]))


def merge(came, mine):
    return pl.pallas_call(
        merge_body,
        out_shape=jax.ShapeDtypeStruct(came.shape, jnp.bfloat16),
        cost_estimate=cost(1e8, 5e5),
        compiler_params=room(3),
        name="merge",
    )(came, *mine)


def split_body(parts, *refs):
    came, mine, (order, near, far) = refs[:parts], refs[parts:-3], refs[-3:]
    lanes = order.shape[0]
    per = len(mine) // parts
    for n, m in enumerate(mine):
        at = (n % per) * lanes
        both = packed(*merged(came[n // per][:, at : at + lanes], m[...]))
        both = dot(both, order[...]).astype(jnp.bfloat16)
        to = slice(n * lanes // 2, (n + 1) * lanes // 2)
        near[:, to] = both[:, : lanes // 2]
        far[:, to] = both[:, lanes // 2 :]


def split(came, mine, order):
    deep, lanes = came[0].shape
    shape = jax.ShapeDtypeStruct((deep, lanes * len(came) // 2), jnp.bfloat16)
    return pl.pallas_call(
        functools.partial(split_body, len(came)),
        out_shape=[shape] * 2,
        cost_estimate=cost(1e8, 1e6),
        compiler_params=room(6),
        name="split",
    )(*came, *mine, order)


def finish_body(a, b, out_w, gain, hidden_w, bias, score_w, interest, logits):
    rows, _, total = merged(a[...], b[...])
    attended = jnp.concatenate(
        [(r / total[h : h + 1]).astype(jnp.bfloat16) for h, r in enumerate(rows)], axis=0
    )
    found = dot(attended, out_w[...], TN).astype(jnp.bfloat16)
    interest[...] = found
    f = found.astype(jnp.float32)
    normed = f * lax.rsqrt(jnp.mean(f * f, axis=1, keepdims=True) + 1e-6) * gain[...]
    v = dot(normed.astype(jnp.bfloat16), hidden_w[...]) + bias[...]
    hidden = (v / (1.0 + jnp.exp(-v))).astype(jnp.bfloat16)
    row = dot(jnp.broadcast_to(score_w[...], (16, v.shape[1])), hidden, NT)[0:1]
    users, cand = logits.shape
    lane = lax.broadcasted_iota(jnp.int32, (users, users * cand), 1)
    mine = lane // cand == lax.broadcasted_iota(jnp.int32, (users, users * cand), 0)
    fold = lax.broadcasted_iota(jnp.int32, (users * cand, cand), 0) % cand
    fold = (fold == lax.broadcasted_iota(jnp.int32, (users * cand, cand), 1)).astype(jnp.bfloat16)
    folded = [dot(jnp.where(mine, r, 0.0).astype(jnp.bfloat16), fold) for r in parts_of(row)]
    logits[...] = folded[0] + folded[1] + folded[2]


def finish(users, a, b, out_w, gain, hidden_w, bias, score_w):
    width, wide = hidden_w.shape
    lanes = a.shape[1]
    return pl.pallas_call(
        finish_body,
        out_shape=[
            jax.ShapeDtypeStruct((lanes, width), jnp.bfloat16),
            jax.ShapeDtypeStruct((users, lanes // users), jnp.float32),
        ],
        cost_estimate=cost(2e8, 1e6),
        compiler_params=room(8),
        name="finish",
    )(a, b, out_w, gain.reshape(1, width), hidden_w, bias.reshape(1, wide), score_w.reshape(1, wide))


def reorder(shape, axes):
    size = 1
    for n in shape:
        size *= n
    spot = lax.broadcasted_iota(jnp.int32, (size, size), 1)
    dims = [shape[a] for a in axes]
    digits = []
    for n in reversed(dims):
        digits.insert(0, spot % n)
        spot = spot // n
    source = 0
    for a, n in enumerate(shape):
        source = source * n + digits[axes.index(a)]
    return (lax.broadcasted_iota(jnp.int32, (size, size), 0) == source).astype(jnp.bfloat16)


def solution(mesh):
    peers = mesh.shape["seq"]
    chips = peers // 2
    slots = chips // 2
    near = lambda d, c: (d % chips) * 2 + c
    ring = [(near(d, 0), near(d + 1, 0)) for d in range(chips)] + [(near(d, 1), near(d - 1, 1)) for d in range(chips)]
    tail = [(near(d, 1), near(d - 1, 1)) for d in range(chips)]
    swap = [(near(d, c), near(d, 1 - c)) for d in range(chips) for c in range(2)]
    back = lambda pairs: [(b, a) for a, b in pairs]

    def on_device(
        candidates,
        codes,
        scale_index,
        lengths,
        scale_table,
        query_weight,
        key_weight,
        value_weight,
        out_weight,
        norm_gain,
        hidden_weight,
        hidden_bias,
        score_weight,
    ):
        users, cand, width = candidates.shape
        places = scale_index.shape[1]
        send = lambda array, pairs: lax.ppermute(array, "seq", pairs)
        me = lax.axis_index("seq")
        mate = me + 1 - 2 * (me % 2)
        starts = jnp.stack([me, mate])[:, None] * places
        live = jnp.clip((lengths[None, :] - starts) // GRAIN, 0, places // GRAIN).astype(jnp.int32)
        live = jnp.concatenate([live, jnp.full((1, users), me % 2, jnp.int32)])

        mine = query_rows(candidates.reshape(users * cand, width), query_weight).reshape(users, cand, width)
        hops = [mine, send(mine, swap)]
        for hop in range(1, slots + 1):
            for _ in range(2):
                hops.append(send(hops[-2], ring if hop < slots else tail))

        value_wt = value_weight.T
        own = history_rows(codes, scale_index, scale_table)
        other = send(own, swap)
        k_own, v_own = project(own, key_weight, value_wt)
        k_other, v_other = project(other, key_weight, value_wt)

        order = reorder((GROUP, SPAN, 2 * cand), (1, 0, 2))
        partial = []
        for block, groups in ((0, 1), (1, users // PARTS // GROUP)):
            calls = []
            for call in range(users // (groups * GROUP)):
                base = call * groups * GROUP
                near_hops = hops[2 * block * SPAN : 2 * (block + 1) * SPAN + 2]
                calls.append(attend(base, groups, live, near_hops, k_own, k_other, v_own, v_other, order))
            partial.append(calls)

        def result(part, slot):
            calls = partial[slot // SPAN]
            per = len(calls) // PARTS
            return [c[slot % SPAN] for c in calls[part * per : (part + 1) * per]]

        come = [result(part, slots - 1)[0] for part in range(PARTS)]
        for slot in range(slots - 2, -1, -1):
            come = [send(c, back(ring)) for c in come]
            if slot:
                come = [merge(c, result(part, slot)) for part, c in enumerate(come)]
        halves = reorder((GROUP, 2, cand), (1, 0, 2))
        first, second = split(come, [x for part in range(PARTS) for x in result(part, 0)], halves)
        moved = [send(x, back(tail)) for x in (first, second)]
        kept, given = (jnp.where(me % 2 == 0, x, y) for x, y in zip((first, second), moved))
        first, second = kept, send(given, swap)
        interest, logits = finish(
            users, first, second, out_weight, norm_gain, hidden_weight, hidden_bias, score_weight
        )
        return interest.reshape(users, cand, width), logits

    in_specs = (
        P("groups", "seq", None),
        P("groups", "seq", None),
        P("groups", "seq"),
        P("groups"),
    ) + (P(),) * 9
    out_specs = (P("groups", "seq", None), P("groups", "seq"))

    return jax.shard_map(on_device, mesh=mesh, in_specs=in_specs, out_specs=out_specs, check_vma=False)
```
